256 devices in a mesh: group: 4 (over y, x), space: 64 (over z, core).
Axes of the slice: x: 2, y: 2, z: 32, core: 2. Of those that a mesh axis runs over, the one named last changes fastest.
The devices are a block of a 4x8x32 slice.
Arguments:
- images: float32 [8, 128, 128, 128], P('group', 'space'), parts along dimension 0, may hold values from -2.7 to 2.7
- weights: float32 [8, 2], P('group'), parts along dimension 0, may hold values from 0 to 1
Outputs:
- relaxed: float32 [8, 128, 128, 128], P('group', 'space'), parts along dimension 0
- spacing: float32 [8, 1], P('group'), parts along dimension 0
The draws below stay inside these ranges and needn't reach their ends.
There are 4 independent parts, one for each index of `group`. The reference program is written for one: setup_inputs(seed, part) draws one part's arguments, and reference() takes and returns one part's arrays. A program takes and returns all parts, laid end to end along the dimension named above; each array names one. Nothing has to cross between parts.
All inputs are finite; a program needn't handle non-finite values.
Results may differ from the reference program's by a relative error of at most 0.0002.
Values sent between devices are 32-bit elements; how exact they have to be, the bound alone decides.
A program may use at most 64 MiB of HBM per device.

```python
import math
import jax
import jax.numpy as jnp
from jax import lax

LX = 128
LY = 128
LZ = 128
IMAGES = 2
ITERS = 2


def correlated_rows(noise):
    total = noise
    for offset in range(1, 16):
        total = total + jnp.roll(noise, offset, axis=1)
    return total * 0.25


def draw_images(key, part):
    extent = (IMAGES, LX, LY, LZ)
    first_key = jax.random.fold_in(key, 0)
    third_key = jax.random.fold_in(key, 2)
    ramp = jnp.arange(LX, dtype=jnp.float32) / (LX - 1)
    amplitude = (0.3 * jnp.exp(ramp * math.log(3.0)))[None, :, None, None]
    parity = (jnp.arange(LX, dtype=jnp.int32) % 2).astype(jnp.float32)
    alternation = (1.0 - 2.0 * parity)[None, :, None, None]
    coherent = jax.random.truncated_normal(first_key, -3.0, 3.0, extent, jnp.float32)
    white_noise = jax.random.truncated_normal(third_key, -3.0, 3.0, extent, jnp.float32)
    rough_part = jnp.clip(alternation * (0.85 * correlated_rows(coherent)) + 0.5 * white_noise, -3.0, 3.0)
    return amplitude * rough_part


def draw_weights(key, part):
    fractions = jax.random.uniform(key, (IMAGES,), jnp.float32, 0.1, 0.9)
    active = (jnp.arange(IMAGES, dtype=jnp.int32) < IMAGES - 1).astype(jnp.float32)
    fractions = fractions * active
    diagonal = jnp.eye(IMAGES, dtype=jnp.float32) * (1.0 - fractions)[:, None]
    upper = jnp.eye(IMAGES, k=1, dtype=jnp.float32) * fractions[:, None]
    return diagonal + upper


def setup_inputs(seed: int = 0, part: int = 0) -> dict:
    arg_keys = jax.random.split(jax.random.key(seed), 3)
    part_splits = jax.random.split(jax.random.fold_in(arg_keys[2], part), 3)
    return {
        "images": draw_images(jax.random.fold_in(jax.random.fold_in(arg_keys[2], part), 71), part),
        "weights": draw_weights(jax.random.fold_in(jax.random.fold_in(arg_keys[2], part), 71), part),
    }


time_step = 0.1
gradient_weight = 1.0


def wave_squares(length):
    indices = jnp.arange(length, dtype=jnp.int32)
    signed = jnp.where(indices <= length // 2, indices, indices - length)
    number = signed.astype(jnp.float32) * (2.0 * math.pi / length)
    return number * number


def reference(images, weights):
    squares = wave_squares(LX)[:, None, None] + wave_squares(LY)[None, :, None] + wave_squares(LZ)[None, None, :]
    damping = 1.0 / (1.0 + time_step * gradient_weight * squares * squares)
    coupling = time_step * squares * damping
    cell_count = LX * LY * LZ
    concentration = images
    spacings = []
    for iteration in range(ITERS):
        potential = concentration * concentration * concentration - concentration
        spectrum = jnp.fft.fftn(concentration, axes=(1, 2, 3)) * damping - jnp.fft.fftn(potential, axes=(1, 2, 3)) * coupling
        concentration = jnp.real(jnp.fft.ifftn(spectrum, axes=(1, 2, 3))).astype(jnp.float32)
        difference = concentration[1:] - concentration[:-1]
        spacings.append(jnp.sum(difference * difference, axis=(1, 2, 3)) / cell_count)
        concentration = jnp.einsum('ij,jxyz->ixyz', weights, concentration, precision=lax.Precision.HIGHEST)
    return concentration, jnp.stack(spacings)
```

```python
import functools
import math

import jax
import jax.numpy as jnp
import numpy as np
from jax import lax
from jax.experimental import pallas as pl
from jax.experimental.pallas import tpu as pltpu
from jax.sharding import PartitionSpec as P

ITERS = 2
CORES = 2
SUBLANES = 8
time_step = 0.1
gradient_weight = 1.0


def frequencies(length):
    half = length // 2
    return np.concatenate([np.arange(half), [half], np.arange(1, half)])


def real_basis(length):
    half = length // 2
    cells = np.arange(length)
    product = np.outer(frequencies(length), cells) % length
    angles = product * (2.0 * math.pi / length)
    rows = np.where(np.arange(length)[:, None] <= half, np.cos(angles), np.sin(angles)) * math.sqrt(2.0 / length)
    rows[[0, half]] *= math.sqrt(0.5)
    return rows


def wave_squares(length):
    return (frequencies(length) * (2.0 * math.pi / length)) ** 2


def split(value):
    high = value.astype(jnp.bfloat16)
    return high, (value - high.astype(jnp.float32)).astype(jnp.bfloat16)


def product(left, right):
    dot = functools.partial(jnp.dot, preferred_element_type=jnp.float32)
    return dot(left[0], right[0]) + (dot(left[0], right[1]) + dot(left[1], right[0]))


def kernel(
    shape, axis_size,
    images_ref, weights_ref, qy_ref, qyt_ref, qz_ref, qzt_ref, qx_ref, qxt_ref, sqx_ref, sqz_ref,
    out_ref, spacing_ref,
    first_send, first_recv, back_send, back_recv, next_send, next_recv, last_send, last_recv,
    part_send, part_recv, field_spectrum, send_sem, recv_sem,
):
    image_count, planes, second_length, third_length = shape
    half = second_length // 2
    chips = axis_size // CORES
    me = lax.axis_index("space")
    group = lax.axis_index("group")
    my_chip, my_core = me // CORES, me % CORES

    def partner(offset, core):
        return lax.rem(my_chip + offset + chips, chips) * CORES + core

    barrier = pltpu.get_barrier_semaphore()

    def greet(step, carry):
        pl.semaphore_signal(
            barrier, inc=1, device_id=(group, lax.rem(me + step, axis_size)), device_id_type=pl.DeviceIdType.MESH
        )
        return carry

    lax.fori_loop(1, axis_size, greet, 0)

    def exchange(send, recv, phase):
        def copy_to(target):
            pltpu.make_async_remote_copy(
                src_ref=send.at[target],
                dst_ref=recv.at[me],
                send_sem=send_sem.at[phase],
                recv_sem=recv_sem.at[phase],
                device_id=(group, target),
                device_id_type=pl.DeviceIdType.MESH,
            ).start()

        copy_to(partner(chips // 2, my_core))
        copy_to(partner(chips // 2, 1 - my_core))

        def step(i, carry):
            distance = chips // 2 - 1 - i
            copy_to(partner(distance, my_core))
            copy_to(partner(-distance, my_core))
            copy_to(partner(distance, 1 - my_core))
            copy_to(partner(-distance, 1 - my_core))
            return carry

        lax.fori_loop(0, chips // 2 - 1, step, 0)
        copy_to(partner(0, 1 - my_core))

    def finish(send, recv, phase):
        others = pl.ds(0, axis_size - 1)
        pltpu.make_async_copy(recv.at[others], recv.at[others], recv_sem.at[phase]).wait()
        pltpu.make_async_copy(send.at[others], send.at[others], send_sem.at[phase]).wait()

    def rows_of(field, image, plane, parity):
        return ((field * image_count + image) * planes + plane) * 2 + parity

    def spread(send, row, value):
        send[:, row // SUBLANES, row % SUBLANES, :] = value

    def gathered(recv, row):
        return recv[:, row // SUBLANES, row % SUBLANES, :]

    qy, qyt = (qy_ref[0], qy_ref[1]), (qyt_ref[0], qyt_ref[1])
    qz, qzt = (qz_ref[0], qz_ref[1]), (qzt_ref[0], qzt_ref[1])
    qx, qxt = (qx_ref[0], qx_ref[1]), (qxt_ref[0], qxt_ref[1])

    def forward_slab(value, send, field, image, plane):
        along_third = product(split(value), qzt)
        spectrum = product(qy, split(along_third))
        for parity in range(2):
            spread(send, rows_of(field, image, plane, parity), spectrum[parity * half : (parity + 1) * half])

    def backward_slab(recv, image, plane):
        spectrum = jnp.concatenate([gathered(recv, rows_of(0, image, plane, parity)) for parity in range(2)], 0)
        along_second = product(qyt, split(spectrum))
        return product(split(along_second), qz)

    def forward_pencils(recv, field):
        columns = [
            jnp.concatenate([gathered(recv, rows_of(field, image, plane, parity)) for plane in range(planes)], 0)
            for image in range(image_count)
            for parity in range(2)
        ]
        return product(qx, split(jnp.concatenate(columns, 1)))

    def backward_pencils(spectrum, send):
        columns = product(qxt, split(spectrum))
        for image in range(image_count):
            for plane in range(planes):
                for parity in range(2):
                    start = (image * 2 + parity) * third_length
                    spread(
                        send, rows_of(0, image, plane, parity),
                        columns[plane * axis_size : (plane + 1) * axis_size, start : start + third_length],
                    )

    def potential(value):
        return value * value * value - value

    for image in range(image_count):
        for plane in range(planes):
            value = images_ref[image, plane]
            forward_slab(value, first_send, 0, image, plane)
            forward_slab(potential(value), first_send, 1, image, plane)
    first_recv[me] = first_send[me]
    pl.semaphore_wait(barrier, axis_size - 1)
    exchange(first_send, first_recv, 0)

    number = 2.0 * math.pi / second_length
    cosine_number = me.astype(jnp.float32) * number
    other_number = jnp.where(me == 0, jnp.float32(half), me.astype(jnp.float32)) * number
    squares = jnp.concatenate(
        [sqx_ref[...] + sqz_ref[...] + square for square in (cosine_number * cosine_number, other_number * other_number)], 1
    )
    damping = 1.0 / (1.0 + time_step * gradient_weight * squares * squares)
    coupling = time_step * squares * damping
    width = 2 * third_length

    def image_of(value, image):
        return value[:, image * width : (image + 1) * width]

    def mixed(values):
        new = []
        for i in range(image_count):
            total = weights_ref[i, 0] * values[0]
            for j in range(1, image_count):
                total = total + weights_ref[i, j] * values[j]
            new.append(total)
        return new

    def new_spectra(field_parts, potential_parts):
        return [damping * field_parts[i] - coupling * image_of(potential_parts, i) for i in range(image_count)]

    lane = lax.broadcasted_iota(jnp.int32, (1, third_length), 1)

    def spacing_parts(values, row, iteration):
        for j in range(image_count - 1):
            difference = values[j + 1] - values[j]
            row = jnp.where(lane == iteration * (image_count - 1) + j, jnp.sum(difference * difference), row)
        return row

    finish(first_send, first_recv, 0)
    field_parts = forward_pencils(first_recv, 0)
    spectra = new_spectra([image_of(field_parts, i) for i in range(image_count)], forward_pencils(first_recv, 1))
    parts = spacing_parts(spectra, jnp.zeros((1, third_length), jnp.float32), 0)
    spectra = mixed(spectra)
    backward_pencils(jnp.concatenate(spectra, 1), back_send)
    back_recv[me] = back_send[me]
    exchange(back_send, back_recv, 1)
    field_spectrum[...] = jnp.concatenate(spectra, 1)

    finish(back_send, back_recv, 1)
    for image in range(image_count):
        for plane in range(planes):
            forward_slab(potential(backward_slab(back_recv, image, plane)), next_send, 0, image, plane)
    next_recv[me] = next_send[me]
    exchange(next_send, next_recv, 2)

    finish(next_send, next_recv, 2)
    spectra = new_spectra([image_of(field_spectrum, i) for i in range(image_count)], forward_pencils(next_recv, 0))
    part_send[0] = spacing_parts(spectra, parts, 1)
    backward_pencils(jnp.concatenate(mixed(spectra), 1), last_send)
    last_recv[me] = last_send[me]

    def part_to(step, carry):
        target = lax.rem(me + step, axis_size)
        pltpu.make_async_remote_copy(
            src_ref=part_send.at[0],
            dst_ref=part_recv.at[me],
            send_sem=send_sem.at[4],
            recv_sem=recv_sem.at[4],
            device_id=(group, target),
            device_id_type=pl.DeviceIdType.MESH,
        ).start()
        return carry

    lax.fori_loop(1, axis_size, part_to, 0)
    part_recv[me] = part_send[0]
    exchange(last_send, last_recv, 3)

    finish(last_send, last_recv, 3)
    for image in range(image_count):
        for plane in range(planes):
            out_ref[image, plane] = backward_slab(last_recv, image, plane)
    others = pl.ds(0, axis_size - 1)
    pltpu.make_async_copy(part_recv.at[others], part_recv.at[others], recv_sem.at[4]).wait()
    pltpu.make_async_copy(part_recv.at[others], part_recv.at[others], send_sem.at[4]).wait()
    cell_count = planes * axis_size * second_length * third_length
    totals = jnp.sum(part_recv[...], axis=0) / cell_count
    for iteration in range(ITERS):
        first = iteration * (image_count - 1)
        spacing_ref[iteration : iteration + 1, :] = totals[:, first : first + image_count - 1]


def two_parts(matrix):
    matrix = matrix.astype(np.float32)
    high = matrix.astype(jnp.bfloat16)
    low = (matrix - high.astype(np.float32)).astype(jnp.bfloat16)
    return np.stack([high, low])


def local(axis_size, images, weights):
    image_count, planes, second_length, third_length = images.shape
    first_length = planes * axis_size
    assert second_length == 2 * axis_size and axis_size % (2 * CORES) == 0
    basis_x = real_basis(first_length)
    order = np.arange(first_length).reshape(axis_size, planes).T.reshape(-1)
    basis_x = basis_x[:, order]
    basis_y, basis_z = real_basis(second_length), real_basis(third_length)
    tables = [two_parts(m) for m in (basis_y, basis_y.T, basis_z, basis_z.T, basis_x, basis_x.T)]
    squares_x = np.repeat(wave_squares(first_length)[:, None], third_length, 1).astype(np.float32)
    squares_z = wave_squares(third_length)[None, :].astype(np.float32)

    tiles = image_count * planes * 2 // SUBLANES
    assert tiles * SUBLANES == image_count * planes * 2
    chunk = lambda count: pltpu.VMEM((axis_size, count, SUBLANES, third_length), jnp.float32)
    assert ITERS * (image_count - 1) <= third_length
    vmem = pl.BlockSpec(memory_space=pltpu.VMEM)
    return pl.pallas_call(
        functools.partial(kernel, images.shape, axis_size),
        out_shape=(
            jax.ShapeDtypeStruct(images.shape, jnp.float32),
            jax.ShapeDtypeStruct((ITERS, image_count - 1), jnp.float32),
        ),
        in_specs=[vmem, pl.BlockSpec(memory_space=pltpu.SMEM)] + [vmem] * 8,
        out_specs=(vmem, vmem),
        scratch_shapes=[
            chunk(2 * tiles), chunk(2 * tiles),
            chunk(tiles), chunk(tiles), chunk(tiles), chunk(tiles), chunk(tiles), chunk(tiles),
            pltpu.VMEM((1, 1, third_length), jnp.float32),
            pltpu.VMEM((axis_size, 1, third_length), jnp.float32),
            pltpu.VMEM((first_length, image_count * 2 * third_length), jnp.float32),
            pltpu.SemaphoreType.DMA((5,)),
            pltpu.SemaphoreType.DMA((5,)),
        ],
        compiler_params=pltpu.CompilerParams(collective_id=0, has_side_effects=True, vmem_limit_bytes=32 * 1024 * 1024),
    )(images, weights, *[jnp.asarray(t) for t in tables], jnp.asarray(squares_x), jnp.asarray(squares_z))


def solution(mesh):
    return jax.shard_map(
        functools.partial(local, mesh.shape["space"]),
        mesh=mesh,
        in_specs=(P("group", "space", None, None), P("group", None)),
        out_specs=(P("group", "space", None, None), P("group", None)),
        check_vma=False,
    )
```

```python
import functools
import math

import jax
import jax.numpy as jnp
import numpy as np
from jax import lax
from jax.experimental import pallas as pl
from jax.experimental.pallas import tpu as pltpu
from jax.sharding import PartitionSpec as P

ITERS = 2
CORES = 2
TABLES = 6
time_step = 0.1
gradient_weight = 1.0


def frequencies(length):
    half = length // 2
    return np.concatenate([np.arange(half), [half], np.arange(1, half)])


def real_basis(length):
    half = length // 2
    cells = np.arange(length)
    product = np.outer(frequencies(length), cells) % length
    angles = product * (2.0 * math.pi / length)
    rows = np.where(np.arange(length)[:, None] <= half, np.cos(angles), np.sin(angles)) * math.sqrt(2.0 / length)
    rows[[0, half]] *= math.sqrt(0.5)
    return rows


def split(value):
    high = value.astype(jnp.bfloat16)
    return high, (value - high.astype(jnp.float32)).astype(jnp.bfloat16)


def product(left, right):
    dot = functools.partial(jnp.dot, preferred_element_type=jnp.float32)
    return dot(left[0], right[0]) + (dot(left[0], right[1]) + dot(left[1], right[0]))


def kernel(
    shape, axis_size,
    images_hbm, weights_hbm, *refs,
):
    tables_hbm, refs = refs[:TABLES], refs[TABLES:]
    out_ref, spacing_ref, images_ref, weights_ref = refs[:4]
    tables, refs = refs[4 : 4 + TABLES], refs[4 + TABLES :]
    (
        first_send, first_recv, back_send, back_recv, next_send, next_recv, last_send, last_recv,
        part_send, part_recv, field_spectrum, load_sem, send_sem, recv_sem,
    ) = refs
    image_count, planes, second_length, third_length = shape
    first_length = planes * axis_size
    half = second_length // 2
    chips = axis_size // CORES
    me = lax.axis_index("space")
    group = lax.axis_index("group")
    my_chip, my_core = me // CORES, lax.rem(me, CORES)
    both = image_count * planes

    def partner(offset, core):
        return lax.rem(my_chip + offset + chips, chips) * CORES + core

    def farthest_first(visit):
        visit(partner(chips // 2, my_core))
        visit(partner(chips // 2, 1 - my_core))

        def step(i, carry):
            distance = chips // 2 - 1 - i
            visit(partner(distance, my_core))
            visit(partner(-distance, my_core))
            visit(partner(distance, 1 - my_core))
            visit(partner(-distance, 1 - my_core))
            return carry

        lax.fori_loop(0, chips // 2 - 1, step, 0)
        visit(partner(0, 1 - my_core))

    barrier = pltpu.get_barrier_semaphore()
    farthest_first(
        lambda target: pl.semaphore_signal(
            barrier, inc=1, device_id=(group, target), device_id_type=pl.DeviceIdType.MESH
        )
    )
    loads = [
        pltpu.make_async_copy(source, target, load_sem.at[i])
        for i, (source, target) in enumerate(
            zip((images_hbm, weights_hbm, *tables_hbm), (images_ref, weights_ref, *tables))
        )
    ]
    for load in loads:
        load.start()

    def exchange(send, recv, rows, phase):
        recv[me, rows] = send[me, rows]

        def copy_to(target):
            pltpu.make_async_remote_copy(
                src_ref=send.at[target, rows],
                dst_ref=recv.at[me, rows],
                send_sem=send_sem.at[phase],
                recv_sem=recv_sem.at[phase],
                device_id=(group, target),
                device_id_type=pl.DeviceIdType.MESH,
            ).start()

        farthest_first(copy_to)

    def finish(recv, rows, phase):
        arrived = recv.at[pl.ds(0, axis_size - 1), rows]
        pltpu.make_async_copy(arrived, arrived, recv_sem.at[phase]).wait()

    def drain(send, rows, phase):
        sent = send.at[pl.ds(0, axis_size - 1), rows]
        pltpu.make_async_copy(sent, sent, send_sem.at[phase]).wait()

    def matrix(k):
        return tables[k][0], tables[k][1]

    qy, qyt, qz, qzt, qx, qxt = [lambda k=k: matrix(k) for k in range(TABLES)]

    def forward_slab(value):
        return product(qy(), split(product(split(value), qzt())))

    def backward_slab(recv, even_row, odd_row):
        spectrum = jnp.concatenate([recv[:, even_row, :], recv[:, odd_row, :]], 0)
        return product(split(product(qyt(), split(spectrum))), qz())

    def pencils(recv, rows):
        return jnp.concatenate([recv[:, row, :] for row in rows], 0)

    def forward_pencils(columns):
        return product(qx(), split(jnp.concatenate(columns, 1)))

    def potential(value):
        return value * value * value - value

    def first_row(parity, field, image, plane):
        return parity * 2 * both + (field * image_count + image) * planes + plane

    def back_row(parity, image, plane):
        return (parity * image_count + image) * planes + plane

    def next_row(image, parity, plane):
        return (image * 2 + parity) * planes + plane

    for load in loads:
        load.wait()
    for image in range(image_count):
        for plane in range(planes):
            value = images_ref[image, plane]
            for field, part in enumerate((value, potential(value))):
                spectrum = forward_slab(part)
                for parity in range(2):
                    first_send[:, first_row(parity, field, image, plane), :] = spectrum[parity * half : (parity + 1) * half]
    pl.semaphore_wait(barrier, axis_size - 1)
    first_rows = [pl.ds(parity * 2 * both, 2 * both) for parity in range(2)]
    for parity in range(2):
        exchange(first_send, first_recv, first_rows[parity], parity)

    def squares_of(index, length):
        frequency = jnp.where(index <= length // 2, index, index - length // 2).astype(jnp.float32)
        number = frequency * (2.0 * math.pi / length)
        return number * number

    square_x = squares_of(lax.broadcasted_iota(jnp.int32, (first_length, third_length), 0), first_length)
    square_z = squares_of(lax.broadcasted_iota(jnp.int32, (first_length, third_length), 1), third_length)
    my_rows = jnp.full((first_length, third_length), me, jnp.int32)
    frequencies_y = (my_rows, jnp.where(my_rows == 0, half, my_rows))
    damping, coupling = [], []
    for frequency in frequencies_y:
        number = frequency.astype(jnp.float32) * (2.0 * math.pi / second_length)
        squares = square_x + number * number + square_z
        damping.append(1.0 / (1.0 + time_step * gradient_weight * squares * squares))
        coupling.append(time_step * squares * damping[-1])

    weight = [[weights_ref[i : i + 1, j : j + 1] for j in range(image_count)] for i in range(image_count)]

    def mixed(values):
        new = []
        for i in range(image_count):
            total = weight[i][0] * values[0]
            for j in range(1, image_count):
                total = total + weight[i][j] * values[j]
            new.append(total)
        return new

    def columns_of(value, k):
        return value[:, k * third_length : (k + 1) * third_length]

    lane = lax.broadcasted_iota(jnp.int32, (1, third_length), 1)

    def spacing_parts(values, row, iteration):
        for j in range(image_count - 1):
            difference = values[j + 1] - values[j]
            row = row + jnp.where(lane == iteration * (image_count - 1) + j, jnp.sum(difference * difference), 0.0)
        return row

    parts = jnp.zeros((1, third_length), jnp.float32)
    back_chunks = [(0, pl.ds(0, both), 2)] + [
        (1, pl.ds(both + image * planes, planes), 3 + image) for image in range(image_count)
    ]
    for parity in range(2):
        finish(first_recv, first_rows[parity], parity)
        spectra = forward_pencils([
            pencils(first_recv, [first_row(parity, field, image, plane) for plane in range(planes)])
            for field in range(2)
            for image in range(image_count)
        ])
        new = [
            damping[parity] * columns_of(spectra, image) - coupling[parity] * columns_of(spectra, image_count + image)
            for image in range(image_count)
        ]
        parts = spacing_parts(new, parts, 0)
        new = mixed(new)
        for image in range(image_count):
            field_spectrum[image, parity] = new[image]
        values = product(qxt(), split(jnp.concatenate(new, 1)))
        for image in range(image_count):
            for plane in range(planes):
                back_send[:, back_row(parity, image, plane), :] = columns_of(values, image)[
                    plane * axis_size : (plane + 1) * axis_size
                ]
        for chunk_parity, rows, phase in back_chunks:
            if chunk_parity == parity:
                exchange(back_send, back_recv, rows, phase)

    image_rows = [pl.ds(image * 2 * planes, 2 * planes) for image in range(image_count)]
    finish(back_recv, back_chunks[0][1], back_chunks[0][2])
    for image in range(image_count):
        finish(back_recv, back_chunks[1 + image][1], back_chunks[1 + image][2])
        for plane in range(planes):
            value = backward_slab(back_recv, back_row(0, image, plane), back_row(1, image, plane))
            spectrum = forward_slab(potential(value))
            for parity in range(2):
                next_send[:, next_row(image, parity, plane), :] = spectrum[parity * half : (parity + 1) * half]
        exchange(next_send, next_recv, image_rows[image], 3 + image_count + image)

    part_phase = 3 + 3 * image_count
    spectra = []
    for image in range(image_count):
        finish(next_recv, image_rows[image], 3 + image_count + image)
        changes = forward_pencils([
            pencils(next_recv, [next_row(image, parity, plane) for plane in range(planes)]) for parity in range(2)
        ])
        new = [
            damping[parity] * field_spectrum[image, parity] - coupling[parity] * columns_of(changes, parity)
            for parity in range(2)
        ]
        new = jnp.concatenate(new, 1)
        spectra.append(new)
        if image == image_count - 1:
            part_send[0] = spacing_parts(spectra, parts, 1)
            part_recv[me] = part_send[0]
            farthest_first(
                lambda target: pltpu.make_async_remote_copy(
                    src_ref=part_send.at[0],
                    dst_ref=part_recv.at[me],
                    send_sem=send_sem.at[part_phase],
                    recv_sem=recv_sem.at[part_phase],
                    device_id=(group, target),
                    device_id_type=pl.DeviceIdType.MESH,
                ).start()
            )
        values = product(qxt(), split(new))
        for parity in range(2):
            for plane in range(planes):
                last_send[:, next_row(image, parity, plane), :] = columns_of(values, parity)[
                    plane * axis_size : (plane + 1) * axis_size
                ]
        exchange(last_send, last_recv, image_rows[image], 3 + 2 * image_count + image)

    relaxed = []
    for image in range(image_count):
        if image == image_count - 1:
            arrived = part_recv.at[pl.ds(0, axis_size - 1)]
            pltpu.make_async_copy(arrived, arrived, recv_sem.at[part_phase]).wait()
            cell_count = first_length * second_length * third_length
            totals = jnp.sum(part_recv[...], axis=0) / cell_count
            spacing_ref[...] = totals[:, : ITERS * (image_count - 1)]
        finish(last_recv, image_rows[image], 3 + 2 * image_count + image)
        relaxed.append([
            backward_slab(last_recv, next_row(image, 0, plane), next_row(image, 1, plane)) for plane in range(planes)
        ])
    for plane in range(planes):
        for image, value in enumerate(mixed([relaxed[j][plane] for j in range(image_count)])):
            out_ref[image, plane] = value

    for parity in range(2):
        drain(first_send, first_rows[parity], parity)
    for _, rows, phase in back_chunks:
        drain(back_send, rows, phase)
    for image in range(image_count):
        drain(next_send, image_rows[image], 3 + image_count + image)
        drain(last_send, image_rows[image], 3 + 2 * image_count + image)
    sent = part_recv.at[pl.ds(0, axis_size - 1)]
    pltpu.make_async_copy(sent, sent, send_sem.at[part_phase]).wait()


def two_parts(matrix):
    matrix = matrix.astype(np.float32)
    high = matrix.astype(jnp.bfloat16)
    low = (matrix - high.astype(np.float32)).astype(jnp.bfloat16)
    return np.stack([high, low])


def local(axis_size, images, weights):
    image_count, planes, second_length, third_length = images.shape
    first_length = planes * axis_size
    assert second_length == 2 * axis_size and axis_size % (2 * CORES) == 0
    assert ITERS * (image_count - 1) <= third_length
    basis_x = real_basis(first_length)
    order = np.arange(first_length).reshape(axis_size, planes).T.reshape(-1)
    basis_x = basis_x[:, order]
    basis_y, basis_z = real_basis(second_length), real_basis(third_length)
    tables = [two_parts(m) for m in (basis_y, basis_y.T, basis_z, basis_z.T, basis_x, basis_x.T)]

    rows = image_count * planes * 2
    message = lambda count: pltpu.VMEM((axis_size, count, third_length), jnp.float32)
    phases = 4 + 3 * image_count
    hbm = pl.BlockSpec(memory_space=pltpu.HBM)
    vmem = pl.BlockSpec(memory_space=pltpu.VMEM)
    relaxed, spacing = pl.pallas_call(
        functools.partial(kernel, images.shape, axis_size),
        out_shape=(
            jax.ShapeDtypeStruct(images.shape, jnp.float32),
            jax.ShapeDtypeStruct((1, ITERS * (image_count - 1)), jnp.float32),
        ),
        in_specs=[hbm] * (2 + TABLES),
        out_specs=(vmem, vmem),
        scratch_shapes=[
            pltpu.VMEM(images.shape, jnp.float32),
            pltpu.VMEM(weights.shape, jnp.float32),
            *[pltpu.VMEM(t.shape, jnp.bfloat16) for t in tables],
            message(2 * rows), message(2 * rows),
            message(rows), message(rows), message(rows), message(rows), message(rows), message(rows),
            message(1), message(1),
            pltpu.VMEM((image_count, 2, first_length, third_length), jnp.float32),
            pltpu.SemaphoreType.DMA((2 + TABLES,)),
            pltpu.SemaphoreType.DMA((phases,)),
            pltpu.SemaphoreType.DMA((phases,)),
        ],
        compiler_params=pltpu.CompilerParams(collective_id=0, has_side_effects=True),
    )(images, weights, *[jnp.asarray(t) for t in tables])
    return relaxed, spacing.reshape(ITERS, image_count - 1)


def solution(mesh):
    return jax.shard_map(
        functools.partial(local, mesh.shape["space"]),
        mesh=mesh,
        in_specs=(P("group", "space", None, None), P("group", None)),
        out_specs=(P("group", "space", None, None), P("group", None)),
        check_vma=False,
    )
```

```python
import functools
import math

import jax
import jax.numpy as jnp
import numpy as np
from jax import lax
from jax.experimental import pallas as pl
from jax.experimental.pallas import tpu as pltpu
from jax.sharding import PartitionSpec as P

ITERS = 2
CORES = 2
TABLES = 6
time_step = 0.1
gradient_weight = 1.0


def frequencies(length):
    half = length // 2
    return np.concatenate([np.arange(half), [half], np.arange(1, half)])


def real_basis(length):
    half = length // 2
    cells = np.arange(length)
    product = np.outer(frequencies(length), cells) % length
    angles = product * (2.0 * math.pi / length)
    rows = np.where(np.arange(length)[:, None] <= half, np.cos(angles), np.sin(angles)) * math.sqrt(2.0 / length)
    rows[[0, half]] *= math.sqrt(0.5)
    return rows


def split(value):
    high = value.astype(jnp.bfloat16)
    return high, (value - high.astype(jnp.float32)).astype(jnp.bfloat16)


def product(left, right):
    dot = functools.partial(jnp.dot, preferred_element_type=jnp.float32)
    return dot(left[0], right[0]) + (dot(left[0], right[1]) + dot(left[1], right[0]))


def kernel(
    shape, axis_size,
    images_hbm, weights_hbm, *refs,
):
    tables_hbm, refs = refs[:TABLES], refs[TABLES:]
    out_ref, spacing_ref, images_ref, weights_ref = refs[:4]
    tables, refs = refs[4 : 4 + TABLES], refs[4 + TABLES :]
    (
        first_send, first_recv, back_send, back_recv, next_send, next_recv, last_send, last_recv,
        pair_send, pair_recv, part_send, part_recv, field_spectrum, load_sem, send_sem, recv_sem,
    ) = refs
    image_count, planes, second_length, third_length = shape
    first_length = planes * axis_size
    half = second_length // 2
    chips = axis_size // CORES
    me = lax.axis_index("space")
    group = lax.axis_index("group")
    my_chip, my_core = me // CORES, lax.rem(me, CORES)
    both = image_count * planes

    def partner(offset, core):
        return lax.rem(my_chip + offset + chips, chips) * CORES + core

    def farthest_first(visit):
        visit(partner(chips // 2, my_core))
        visit(partner(chips // 2, 1 - my_core))

        def step(i, carry):
            distance = chips // 2 - 1 - i
            visit(partner(distance, my_core))
            visit(partner(-distance, my_core))
            visit(partner(distance, 1 - my_core))
            visit(partner(-distance, 1 - my_core))
            return carry

        lax.fori_loop(0, chips // 2 - 1, step, 0)
        visit(partner(0, 1 - my_core))

    barrier = pltpu.get_barrier_semaphore()
    farthest_first(
        lambda target: pl.semaphore_signal(
            barrier, inc=1, device_id=(group, target), device_id_type=pl.DeviceIdType.MESH
        )
    )
    loads = [
        pltpu.make_async_copy(source, target, load_sem.at[i])
        for i, (source, target) in enumerate(
            zip((images_hbm, weights_hbm, *tables_hbm), (images_ref, weights_ref, *tables))
        )
    ]
    for load in loads:
        load.start()

    def exchange(send, recv, rows, phase):
        recv[me, rows] = send[me, rows]

        def copy_to(target):
            pltpu.make_async_remote_copy(
                src_ref=send.at[target, rows],
                dst_ref=recv.at[me, rows],
                send_sem=send_sem.at[phase],
                recv_sem=recv_sem.at[phase],
                device_id=(group, target),
                device_id_type=pl.DeviceIdType.MESH,
            ).start()

        farthest_first(copy_to)

    def finish(recv, rows, phase):
        arrived = recv.at[pl.ds(0, axis_size - 1), rows]
        pltpu.make_async_copy(arrived, arrived, recv_sem.at[phase]).wait()

    def drain(send, rows, phase):
        sent = send.at[pl.ds(0, axis_size - 1), rows]
        pltpu.make_async_copy(sent, sent, send_sem.at[phase]).wait()

    def matrix(k):
        return tables[k][0], tables[k][1]

    qy, qyt, qz, qzt, qx, qxt = [lambda k=k: matrix(k) for k in range(TABLES)]

    def forward_slab(value):
        return product(qy(), split(product(split(value), qzt())))

    def backward_slab(recv, even_row, odd_row):
        spectrum = jnp.concatenate([recv[:, even_row, :], recv[:, odd_row, :]], 0)
        return product(split(product(qyt(), split(spectrum))), qz())

    def pencils(recv, rows):
        return jnp.concatenate([recv[:, row, :] for row in rows], 0)

    def forward_pencils(columns):
        return product(qx(), split(jnp.concatenate(columns, 1)))

    def potential(value):
        return value * value * value - value

    def first_row(parity, field, image, plane):
        return parity * 2 * both + (field * image_count + image) * planes + plane

    def row_of(image, parity, plane):
        return (image * 2 + parity) * planes + plane

    for load in loads:
        load.wait()
    for image in range(image_count):
        for plane in range(planes):
            value = images_ref[image, plane]
            for field, part in enumerate((value, potential(value))):
                spectrum = forward_slab(part)
                for parity in range(2):
                    first_send[:, first_row(parity, field, image, plane), :] = spectrum[parity * half : (parity + 1) * half]
    pl.semaphore_wait(barrier, axis_size - 1)
    first_rows = [pl.ds(parity * 2 * both, 2 * both) for parity in range(2)]
    for parity in range(2):
        exchange(first_send, first_recv, first_rows[parity], parity)

    def squares_of(index, length):
        frequency = jnp.where(index <= length // 2, index, index - length // 2).astype(jnp.float32)
        number = frequency * (2.0 * math.pi / length)
        return number * number

    square_x = squares_of(lax.broadcasted_iota(jnp.int32, (first_length, third_length), 0), first_length)
    square_z = squares_of(lax.broadcasted_iota(jnp.int32, (first_length, third_length), 1), third_length)
    my_rows = jnp.full((first_length, third_length), me, jnp.int32)
    frequencies_y = (my_rows, jnp.where(my_rows == 0, half, my_rows))
    damping, coupling = [], []
    for frequency in frequencies_y:
        number = frequency.astype(jnp.float32) * (2.0 * math.pi / second_length)
        squares = square_x + number * number + square_z
        damping.append(1.0 / (1.0 + time_step * gradient_weight * squares * squares))
        coupling.append(time_step * squares * damping[-1])

    weight = [[weights_ref[i : i + 1, j : j + 1] for j in range(image_count)] for i in range(image_count)]

    def mixed(values):
        new = []
        for i in range(image_count):
            total = weight[i][0] * values[0]
            for j in range(1, image_count):
                total = total + weight[i][j] * values[j]
            new.append(total)
        return new

    def columns_of(value, k):
        return value[:, k * third_length : (k + 1) * third_length]

    lane = lax.broadcasted_iota(jnp.int32, (1, third_length), 1)

    def spacing_parts(values, row, iteration):
        for j in range(image_count - 1):
            difference = values[j + 1] - values[j]
            row = row + jnp.where(lane == iteration * (image_count - 1) + j, jnp.sum(difference * difference), 0.0)
        return row

    parts = jnp.zeros((1, third_length), jnp.float32)
    back_chunks = [(0, pl.ds(0, planes), 2), (1, pl.ds(planes, planes), 3)] + [
        (1, pl.ds(image * 2 * planes, 2 * planes), 3 + image) for image in range(1, image_count)
    ]
    for parity in range(2):
        finish(first_recv, first_rows[parity], parity)
        spectra = forward_pencils([
            pencils(first_recv, [first_row(parity, field, image, plane) for plane in range(planes)])
            for field in range(2)
            for image in range(image_count)
        ])
        new = [
            damping[parity] * columns_of(spectra, image) - coupling[parity] * columns_of(spectra, image_count + image)
            for image in range(image_count)
        ]
        parts = spacing_parts(new, parts, 0)
        new = mixed(new)
        for image in range(image_count):
            field_spectrum[image, parity] = new[image]
        values = product(qxt(), split(jnp.concatenate(new, 1)))
        for image in range(image_count):
            for plane in range(planes):
                back_send[:, row_of(image, parity, plane), :] = columns_of(values, image)[
                    plane * axis_size : (plane + 1) * axis_size
                ]
        for chunk_parity, rows, phase in back_chunks:
            if chunk_parity == parity:
                exchange(back_send, back_recv, rows, phase)

    image_rows = [pl.ds(image * 2 * planes, 2 * planes) for image in range(image_count)]
    finish(back_recv, back_chunks[0][1], back_chunks[0][2])
    for image in range(image_count):
        finish(back_recv, back_chunks[1 + image][1], back_chunks[1 + image][2])
        for plane in range(planes):
            value = backward_slab(back_recv, row_of(image, 0, plane), row_of(image, 1, plane))
            spectrum = forward_slab(potential(value))
            for parity in range(2):
                next_send[:, row_of(image, parity, plane), :] = spectrum[parity * half : (parity + 1) * half]
        exchange(next_send, next_recv, image_rows[image], 3 + image_count + image)

    part_phase = 3 + 3 * image_count
    spectra = []
    for image in range(image_count):
        finish(next_recv, image_rows[image], 3 + image_count + image)
        changes = forward_pencils([
            pencils(next_recv, [row_of(image, parity, plane) for plane in range(planes)]) for parity in range(2)
        ])
        new = [
            damping[parity] * field_spectrum[image, parity] - coupling[parity] * columns_of(changes, parity)
            for parity in range(2)
        ]
        new = jnp.concatenate(new, 1)
        spectra.append(new)
        if image == image_count - 1:
            pair_send[...] = spacing_parts(spectra, parts, 1)
            to_other_core = pltpu.make_async_remote_copy(
                src_ref=pair_send,
                dst_ref=pair_recv,
                send_sem=send_sem.at[part_phase + 1],
                recv_sem=recv_sem.at[part_phase + 1],
                device_id=(group, partner(0, 1 - my_core)),
                device_id_type=pl.DeviceIdType.MESH,
            )
            to_other_core.start()
        values = product(qxt(), split(new))
        for parity in range(2):
            for plane in range(planes):
                last_send[:, row_of(image, parity, plane), :] = columns_of(values, parity)[
                    plane * axis_size : (plane + 1) * axis_size
                ]
        if image == image_count - 1:
            to_other_core.wait()
            part_send[...] = pair_send[...] + pair_recv[...]
            part_recv[my_chip] = part_send[...]

            def part_to(step, carry):
                pltpu.make_async_remote_copy(
                    src_ref=part_send,
                    dst_ref=part_recv.at[my_chip],
                    send_sem=send_sem.at[part_phase],
                    recv_sem=recv_sem.at[part_phase],
                    device_id=(group, partner(step, my_core)),
                    device_id_type=pl.DeviceIdType.MESH,
                ).start()
                return carry

            lax.fori_loop(1, chips, part_to, 0)
        exchange(last_send, last_recv, image_rows[image], 3 + 2 * image_count + image)

    relaxed = []
    for image in range(image_count):
        if image == image_count - 1:
            arrived = part_recv.at[pl.ds(0, chips - 1)]
            pltpu.make_async_copy(arrived, arrived, recv_sem.at[part_phase]).wait()
            cell_count = first_length * second_length * third_length
            totals = jnp.sum(part_recv[...], axis=0) / cell_count
            spacing_ref[...] = totals[:, : ITERS * (image_count - 1)]
        finish(last_recv, image_rows[image], 3 + 2 * image_count + image)
        relaxed.append([
            backward_slab(last_recv, row_of(image, 0, plane), row_of(image, 1, plane)) for plane in range(planes)
        ])
    for plane in range(planes):
        for image, value in enumerate(mixed([relaxed[j][plane] for j in range(image_count)])):
            out_ref[image, plane] = value

    for parity in range(2):
        drain(first_send, first_rows[parity], parity)
    for _, rows, phase in back_chunks:
        drain(back_send, rows, phase)
    for image in range(image_count):
        drain(next_send, image_rows[image], 3 + image_count + image)
        drain(last_send, image_rows[image], 3 + 2 * image_count + image)
    sent = part_recv.at[pl.ds(0, chips - 1)]
    pltpu.make_async_copy(sent, sent, send_sem.at[part_phase]).wait()


def two_parts(matrix):
    matrix = matrix.astype(np.float32)
    high = matrix.astype(jnp.bfloat16)
    low = (matrix - high.astype(np.float32)).astype(jnp.bfloat16)
    return np.stack([high, low])


def local(axis_size, images, weights):
    image_count, planes, second_length, third_length = images.shape
    first_length = planes * axis_size
    assert second_length == 2 * axis_size and axis_size % (2 * CORES) == 0
    assert ITERS * (image_count - 1) <= third_length
    basis_x = real_basis(first_length)
    order = np.arange(first_length).reshape(axis_size, planes).T.reshape(-1)
    basis_x = basis_x[:, order]
    basis_y, basis_z = real_basis(second_length), real_basis(third_length)
    tables = [two_parts(m) for m in (basis_y, basis_y.T, basis_z, basis_z.T, basis_x, basis_x.T)]

    rows = image_count * planes * 2
    message = lambda count: pltpu.VMEM((axis_size, count, third_length), jnp.float32)
    row = pltpu.VMEM((1, third_length), jnp.float32)
    phases = 5 + 3 * image_count
    hbm = pl.BlockSpec(memory_space=pltpu.HBM)
    vmem = pl.BlockSpec(memory_space=pltpu.VMEM)
    relaxed, spacing = pl.pallas_call(
        functools.partial(kernel, images.shape, axis_size),
        out_shape=(
            pltpu.VMEM(images.shape, jnp.float32),
            pltpu.VMEM((1, ITERS * (image_count - 1)), jnp.float32),
        ),
        in_specs=[hbm] * (2 + TABLES),
        out_specs=(vmem, vmem),
        scratch_shapes=[
            pltpu.VMEM(images.shape, jnp.float32),
            pltpu.VMEM(weights.shape, jnp.float32),
            *[pltpu.VMEM(t.shape, jnp.bfloat16) for t in tables],
            message(2 * rows), message(2 * rows),
            message(rows), message(rows), message(rows), message(rows), message(rows), message(rows),
            row, row, row, pltpu.VMEM((axis_size // CORES, 1, third_length), jnp.float32),
            pltpu.VMEM((image_count, 2, first_length, third_length), jnp.float32),
            pltpu.SemaphoreType.DMA((2 + TABLES,)),
            pltpu.SemaphoreType.DMA((phases,)),
            pltpu.SemaphoreType.DMA((phases,)),
        ],
        compiler_params=pltpu.CompilerParams(collective_id=0, has_side_effects=True),
    )(images, weights, *[jnp.asarray(t) for t in tables])
    return relaxed, spacing.reshape(ITERS, image_count - 1)


def solution(mesh):
    return jax.shard_map(
        functools.partial(local, mesh.shape["space"]),
        mesh=mesh,
        in_specs=(P("group", "space", None, None), P("group", None)),
        out_specs=(P("group", "space", None, None), P("group", None)),
        check_vma=False,
    )
```

```python
import functools
import math

import jax
import jax.numpy as jnp
import numpy as np
from jax import lax
from jax.experimental import pallas as pl
from jax.experimental.pallas import tpu as pltpu
from jax.sharding import PartitionSpec as P

ITERS = 2
CORES = 2
TABLES = 6
time_step = 0.1
gradient_weight = 1.0


def frequencies(length):
    half = length // 2
    return np.concatenate([np.arange(half), [half], np.arange(1, half)])


def real_basis(length):
    half = length // 2
    cells = np.arange(length)
    product = np.outer(frequencies(length), cells) % length
    angles = product * (2.0 * math.pi / length)
    rows = np.where(np.arange(length)[:, None] <= half, np.cos(angles), np.sin(angles)) * math.sqrt(2.0 / length)
    rows[[0, half]] *= math.sqrt(0.5)
    return rows


def split(value):
    high = value.astype(jnp.bfloat16)
    return high, (value - high.astype(jnp.float32)).astype(jnp.bfloat16)


def product(left, right):
    dot = functools.partial(jnp.dot, preferred_element_type=jnp.float32)
    return dot(left[0], right[0]) + (dot(left[0], right[1]) + dot(left[1], right[0]))


def kernel(
    shape, axis_size,
    images_hbm, weights_hbm, *refs,
):
    tables_hbm, refs = refs[:TABLES], refs[TABLES:]
    out_ref, spacing_ref, images_ref, weights_ref = refs[:4]
    tables, refs = refs[4 : 4 + TABLES], refs[4 + TABLES :]
    (
        first_send, first_recv, back_send, back_recv, next_send, next_recv, last_send, last_recv,
        pair_send, pair_recv, part_send, part_recv, field_spectrum, load_sem, send_sem, recv_sem, ready_sem,
    ) = refs
    image_count, planes, second_length, third_length = shape
    first_length = planes * axis_size
    half = second_length // 2
    chips = axis_size // CORES
    me = lax.axis_index("space")
    group = lax.axis_index("group")
    my_chip, my_core = me // CORES, lax.rem(me, CORES)
    both = image_count * planes

    def partner(offset, core):
        return lax.rem(my_chip + offset + chips, chips) * CORES + core

    def farthest_first(visit):
        visit(partner(chips // 2, my_core))
        visit(partner(chips // 2, 1 - my_core))

        def step(i, carry):
            distance = chips // 2 - 1 - i
            visit(partner(distance, my_core))
            visit(partner(-distance, my_core))
            visit(partner(distance, 1 - my_core))
            visit(partner(-distance, 1 - my_core))
            return carry

        lax.fori_loop(0, chips // 2 - 1, step, 0)
        visit(partner(0, 1 - my_core))

    loads = [
        pltpu.make_async_copy(source, target, load_sem.at[i])
        for i, (source, target) in enumerate(
            zip((images_hbm, weights_hbm, *tables_hbm), (images_ref, weights_ref, *tables))
        )
    ]
    for load in loads:
        load.start()

    def signal(semaphore, target):
        pl.semaphore_signal(semaphore, inc=1, device_id=(group, target), device_id_type=pl.DeviceIdType.MESH)

    neighbours = [(0, 1 - my_core)] + [(offset, core) for offset in (1, -1) for core in (my_core, 1 - my_core)]
    barrier = pltpu.get_barrier_semaphore()
    for offset, core in neighbours:
        signal(barrier, partner(offset, core))
    def sender(send, recv, rows, phase):
        def copy_to(target):
            pltpu.make_async_remote_copy(
                src_ref=send.at[target, rows],
                dst_ref=recv.at[me, rows],
                send_sem=send_sem.at[phase],
                recv_sem=recv_sem.at[phase],
                device_id=(group, target),
                device_id_type=pl.DeviceIdType.MESH,
            ).start()

        return copy_to

    def exchange(send, recv, rows, phase):
        recv[me, rows] = send[me, rows]
        farthest_first(sender(send, recv, rows, phase))

    def opening_exchange(send, recv, rows, phase):
        copy_to = sender(send, recv, rows, phase)
        recv[me, rows] = send[me, rows]
        pl.semaphore_wait(barrier, len(neighbours))

        def tell():
            signal(ready_sem.at[0], partner(1, my_core))
            signal(ready_sem.at[1], partner(-1, my_core))

        def hear():
            for side in range(2):
                pl.semaphore_wait(ready_sem.at[side], 1)

        tell()
        for offset, core in neighbours:
            copy_to(partner(offset, core))

        def step(distance, carry):
            hear()
            tell()
            for core in (my_core, 1 - my_core):
                copy_to(partner(distance, core))
                copy_to(partner(-distance, core))
            return carry

        lax.fori_loop(2, chips // 2, step, 0)
        hear()
        for core in (my_core, 1 - my_core):
            copy_to(partner(chips // 2, core))

    def finish(recv, rows, phase):
        arrived = recv.at[pl.ds(0, axis_size - 1), rows]
        pltpu.make_async_copy(arrived, arrived, recv_sem.at[phase]).wait()

    def drain(send, rows, phase):
        sent = send.at[pl.ds(0, axis_size - 1), rows]
        pltpu.make_async_copy(sent, sent, send_sem.at[phase]).wait()

    def matrix(k):
        return tables[k][0], tables[k][1]

    qy, qyt, qz, qzt, qx, qxt = [lambda k=k: matrix(k) for k in range(TABLES)]

    def forward_slab(value):
        return product(qy(), split(product(split(value), qzt())))

    def backward_slab(recv, even_row, odd_row):
        spectrum = jnp.concatenate([recv[:, even_row, :], recv[:, odd_row, :]], 0)
        return product(split(product(qyt(), split(spectrum))), qz())

    def pencils(recv, rows):
        return jnp.concatenate([recv[:, row, :] for row in rows], 0)

    def forward_pencils(columns):
        return product(qx(), split(jnp.concatenate(columns, 1)))

    def potential(value):
        return value * value * value - value

    def first_row(parity, field, image, plane):
        return parity * 2 * both + (field * image_count + image) * planes + plane

    def row_of(image, parity, plane):
        return (image * 2 + parity) * planes + plane

    for load in loads:
        load.wait()
    for image in range(image_count):
        for plane in range(planes):
            value = images_ref[image, plane]
            for field, part in enumerate((value, potential(value))):
                spectrum = forward_slab(part)
                for parity in range(2):
                    first_send[:, first_row(parity, field, image, plane), :] = spectrum[parity * half : (parity + 1) * half]
    first_rows = [pl.ds(parity * 2 * both, 2 * both) for parity in range(2)]
    opening_exchange(first_send, first_recv, first_rows[0], 0)
    exchange(first_send, first_recv, first_rows[1], 1)

    def squares_of(index, length):
        frequency = jnp.where(index <= length // 2, index, index - length // 2).astype(jnp.float32)
        number = frequency * (2.0 * math.pi / length)
        return number * number

    square_x = squares_of(lax.broadcasted_iota(jnp.int32, (first_length, third_length), 0), first_length)
    square_z = squares_of(lax.broadcasted_iota(jnp.int32, (first_length, third_length), 1), third_length)
    my_rows = jnp.full((first_length, third_length), me, jnp.int32)
    frequencies_y = (my_rows, jnp.where(my_rows == 0, half, my_rows))
    damping, coupling = [], []
    for frequency in frequencies_y:
        number = frequency.astype(jnp.float32) * (2.0 * math.pi / second_length)
        squares = square_x + number * number + square_z
        damping.append(1.0 / (1.0 + time_step * gradient_weight * squares * squares))
        coupling.append(time_step * squares * damping[-1])

    weight = [[weights_ref[i : i + 1, j : j + 1] for j in range(image_count)] for i in range(image_count)]

    def mixed(values):
        new = []
        for i in range(image_count):
            total = weight[i][0] * values[0]
            for j in range(1, image_count):
                total = total + weight[i][j] * values[j]
            new.append(total)
        return new

    def columns_of(value, k):
        return value[:, k * third_length : (k + 1) * third_length]

    lane = lax.broadcasted_iota(jnp.int32, (1, third_length), 1)

    def spacing_parts(values, row, iteration):
        for j in range(image_count - 1):
            difference = values[j + 1] - values[j]
            row = row + jnp.where(lane == iteration * (image_count - 1) + j, jnp.sum(difference * difference), 0.0)
        return row

    parts = jnp.zeros((1, third_length), jnp.float32)
    back_chunks = [(0, pl.ds(0, planes), 2), (1, pl.ds(planes, planes), 3)] + [
        (1, pl.ds(image * 2 * planes, 2 * planes), 3 + image) for image in range(1, image_count)
    ]
    for parity in range(2):
        finish(first_recv, first_rows[parity], parity)
        spectra = forward_pencils([
            pencils(first_recv, [first_row(parity, field, image, plane) for plane in range(planes)])
            for field in range(2)
            for image in range(image_count)
        ])
        new = [
            damping[parity] * columns_of(spectra, image) - coupling[parity] * columns_of(spectra, image_count + image)
            for image in range(image_count)
        ]
        parts = spacing_parts(new, parts, 0)
        new = mixed(new)
        for image in range(image_count):
            field_spectrum[image, parity] = new[image]
        values = product(qxt(), split(jnp.concatenate(new, 1)))
        for image in range(image_count):
            for plane in range(planes):
                back_send[:, row_of(image, parity, plane), :] = columns_of(values, image)[
                    plane * axis_size : (plane + 1) * axis_size
                ]
        for chunk_parity, rows, phase in back_chunks:
            if chunk_parity == parity:
                exchange(back_send, back_recv, rows, phase)

    image_rows = [pl.ds(image * 2 * planes, 2 * planes) for image in range(image_count)]
    finish(back_recv, back_chunks[0][1], back_chunks[0][2])
    for image in range(image_count):
        finish(back_recv, back_chunks[1 + image][1], back_chunks[1 + image][2])
        for plane in range(planes):
            value = backward_slab(back_recv, row_of(image, 0, plane), row_of(image, 1, plane))
            spectrum = forward_slab(potential(value))
            for parity in range(2):
                next_send[:, row_of(image, parity, plane), :] = spectrum[parity * half : (parity + 1) * half]
        exchange(next_send, next_recv, image_rows[image], 3 + image_count + image)

    part_phase = 3 + 3 * image_count
    spectra = []
    for image in range(image_count):
        finish(next_recv, image_rows[image], 3 + image_count + image)
        changes = forward_pencils([
            pencils(next_recv, [row_of(image, parity, plane) for plane in range(planes)]) for parity in range(2)
        ])
        new = [
            damping[parity] * field_spectrum[image, parity] - coupling[parity] * columns_of(changes, parity)
            for parity in range(2)
        ]
        new = jnp.concatenate(new, 1)
        spectra.append(new)
        if image == image_count - 1:
            pair_send[...] = spacing_parts(spectra, parts, 1)
            to_other_core = pltpu.make_async_remote_copy(
                src_ref=pair_send,
                dst_ref=pair_recv,
                send_sem=send_sem.at[part_phase + 1],
                recv_sem=recv_sem.at[part_phase + 1],
                device_id=(group, partner(0, 1 - my_core)),
                device_id_type=pl.DeviceIdType.MESH,
            )
            to_other_core.start()
        values = product(qxt(), split(new))
        for parity in range(2):
            for plane in range(planes):
                last_send[:, row_of(image, parity, plane), :] = columns_of(values, parity)[
                    plane * axis_size : (plane + 1) * axis_size
                ]
        if image == image_count - 1:
            to_other_core.wait()
            part_send[...] = pair_send[...] + pair_recv[...]
            part_recv[my_chip] = part_send[...]

            def part_to(step, carry):
                pltpu.make_async_remote_copy(
                    src_ref=part_send,
                    dst_ref=part_recv.at[my_chip],
                    send_sem=send_sem.at[part_phase],
                    recv_sem=recv_sem.at[part_phase],
                    device_id=(group, partner(step, my_core)),
                    device_id_type=pl.DeviceIdType.MESH,
                ).start()
                return carry

            lax.fori_loop(1, chips, part_to, 0)
        exchange(last_send, last_recv, image_rows[image], 3 + 2 * image_count + image)

    relaxed = []
    for image in range(image_count):
        if image == image_count - 1:
            arrived = part_recv.at[pl.ds(0, chips - 1)]
            pltpu.make_async_copy(arrived, arrived, recv_sem.at[part_phase]).wait()
            cell_count = first_length * second_length * third_length
            totals = jnp.sum(part_recv[...], axis=0) / cell_count
            spacing_ref[...] = totals[:, : ITERS * (image_count - 1)]
        finish(last_recv, image_rows[image], 3 + 2 * image_count + image)
        relaxed.append([
            backward_slab(last_recv, row_of(image, 0, plane), row_of(image, 1, plane)) for plane in range(planes)
        ])
    for plane in range(planes):
        for image, value in enumerate(mixed([relaxed[j][plane] for j in range(image_count)])):
            out_ref[image, plane] = value

    for parity in range(2):
        drain(first_send, first_rows[parity], parity)
    for _, rows, phase in back_chunks:
        drain(back_send, rows, phase)
    for image in range(image_count):
        drain(next_send, image_rows[image], 3 + image_count + image)
        drain(last_send, image_rows[image], 3 + 2 * image_count + image)
    sent = part_recv.at[pl.ds(0, chips - 1)]
    pltpu.make_async_copy(sent, sent, send_sem.at[part_phase]).wait()


def two_parts(matrix):
    matrix = matrix.astype(np.float32)
    high = matrix.astype(jnp.bfloat16)
    low = (matrix - high.astype(np.float32)).astype(jnp.bfloat16)
    return np.stack([high, low])


def local(axis_size, images, weights):
    image_count, planes, second_length, third_length = images.shape
    first_length = planes * axis_size
    assert second_length == 2 * axis_size and axis_size % (2 * CORES) == 0 and axis_size > 4 * CORES
    assert ITERS * (image_count - 1) <= third_length
    basis_x = real_basis(first_length)
    order = np.arange(first_length).reshape(axis_size, planes).T.reshape(-1)
    basis_x = basis_x[:, order]
    basis_y, basis_z = real_basis(second_length), real_basis(third_length)
    tables = [two_parts(m) for m in (basis_y, basis_y.T, basis_z, basis_z.T, basis_x, basis_x.T)]

    rows = image_count * planes * 2
    message = lambda count: pltpu.VMEM((axis_size, count, third_length), jnp.float32)
    row = pltpu.VMEM((1, third_length), jnp.float32)
    phases = 5 + 3 * image_count
    hbm = pl.BlockSpec(memory_space=pltpu.HBM)
    vmem = pl.BlockSpec(memory_space=pltpu.VMEM)
    relaxed, spacing = pl.pallas_call(
        functools.partial(kernel, images.shape, axis_size),
        out_shape=(
            pltpu.VMEM(images.shape, jnp.float32),
            pltpu.VMEM((1, ITERS * (image_count - 1)), jnp.float32),
        ),
        in_specs=[hbm] * (2 + TABLES),
        out_specs=(vmem, vmem),
        scratch_shapes=[
            pltpu.VMEM(images.shape, jnp.float32),
            pltpu.VMEM(weights.shape, jnp.float32),
            *[pltpu.VMEM(t.shape, jnp.bfloat16) for t in tables],
            message(2 * rows), message(2 * rows),
            message(rows), message(rows), message(rows), message(rows), message(rows), message(rows),
            row, row, row, pltpu.VMEM((axis_size // CORES, 1, third_length), jnp.float32),
            pltpu.VMEM((image_count, 2, first_length, third_length), jnp.float32),
            pltpu.SemaphoreType.DMA((2 + TABLES,)),
            pltpu.SemaphoreType.DMA((phases,)),
            pltpu.SemaphoreType.DMA((phases,)),
            pltpu.SemaphoreType.REGULAR((2,)),
        ],
        compiler_params=pltpu.CompilerParams(collective_id=0, has_side_effects=True),
    )(images, weights, *[jnp.asarray(t) for t in tables])
    return relaxed, spacing.reshape(ITERS, image_count - 1)


def solution(mesh):
    return jax.shard_map(
        functools.partial(local, mesh.shape["space"]),
        mesh=mesh,
        in_specs=(P("group", "space", None, None), P("group", None)),
        out_specs=(P("group", "space", None, None), P("group", None)),
        check_vma=False,
    )
```

```python
import functools
import math

import jax
import jax.numpy as jnp
import numpy as np
from jax import lax
from jax.experimental import pallas as pl
from jax.experimental.pallas import tpu as pltpu
from jax.sharding import PartitionSpec as P

ITERS = 2
CORES = 2
TABLES = 6
NEAR = 6
time_step = 0.1
gradient_weight = 1.0


def frequencies(length):
    half = length // 2
    return np.concatenate([np.arange(half), [half], np.arange(1, half)])


def real_basis(length):
    half = length // 2
    cells = np.arange(length)
    product = np.outer(frequencies(length), cells) % length
    angles = product * (2.0 * math.pi / length)
    rows = np.where(np.arange(length)[:, None] <= half, np.cos(angles), np.sin(angles)) * math.sqrt(2.0 / length)
    rows[[0, half]] *= math.sqrt(0.5)
    return rows


def split(value):
    high = value.astype(jnp.bfloat16)
    return high, (value - high.astype(jnp.float32)).astype(jnp.bfloat16)


def product(left, right):
    dot = functools.partial(jnp.dot, preferred_element_type=jnp.float32)
    return dot(left[0], right[0]) + (dot(left[0], right[1]) + dot(left[1], right[0]))


def kernel(
    shape, axis_size,
    images_hbm, weights_hbm, *refs,
):
    tables_hbm, refs = refs[:TABLES], refs[TABLES:]
    out_ref, spacing_ref, images_ref, weights_ref = refs[:4]
    tables, refs = refs[4 : 4 + TABLES], refs[4 + TABLES :]
    (
        first_send, first_recv, back_send, back_recv, next_send, next_recv, last_send, last_recv,
        pair_send, pair_recv, part_send, part_recv, field_spectrum, load_sem, send_sem, recv_sem, told_sem,
    ) = refs
    image_count, planes, second_length, third_length = shape
    first_length = planes * axis_size
    half = second_length // 2
    chips = axis_size // CORES
    me = lax.axis_index("space")
    group = lax.axis_index("group")
    my_chip, my_core = me // CORES, lax.rem(me, CORES)
    both = image_count * planes

    def partner(offset, core):
        return lax.rem(my_chip + offset + chips, chips) * CORES + core

    near = min(NEAR, chips // 2 - 1)

    def farthest_first(visit, beyond=-1):
        visit(partner(chips // 2, my_core))
        visit(partner(chips // 2, 1 - my_core))

        def step(i, carry):
            distance = chips // 2 - 1 - i
            visit(partner(distance, my_core))
            visit(partner(-distance, my_core))
            visit(partner(distance, 1 - my_core))
            visit(partner(-distance, 1 - my_core))
            return carry

        lax.fori_loop(0, chips // 2 - 1 - max(beyond, 0), step, 0)
        if beyond < 0:
            visit(partner(0, 1 - my_core))

    loads = [
        pltpu.make_async_copy(source, target, load_sem.at[i])
        for i, (source, target) in enumerate(
            zip((images_hbm, weights_hbm, *tables_hbm), (images_ref, weights_ref, *tables))
        )
    ]
    for load in loads:
        load.start()

    barrier = pltpu.get_barrier_semaphore()

    def signal(semaphore, target):
        pl.semaphore_signal(semaphore, inc=1, device_id=(group, target), device_id_type=pl.DeviceIdType.MESH)

    def greet(distance, core):
        signal(barrier, partner(distance, core))
        signal(barrier, partner(-distance, core))

    def greet_far(i, carry):
        greet(chips // 2 - 1 - i, 1)
        return carry

    def greet_near(i, carry):
        greet(1 + i, 0)
        greet(1 + i, 1)
        return carry

    signal(barrier, partner(chips // 2, 1))
    lax.fori_loop(0, chips // 2 - 1 - near, greet_far, 0)
    lax.fori_loop(0, near, greet_near, 0)
    signal(barrier, partner(0, 1 - my_core))
    def sender(send, recv, rows, phase):
        def copy_to(target):
            pltpu.make_async_remote_copy(
                src_ref=send.at[target, rows],
                dst_ref=recv.at[me, rows],
                send_sem=send_sem.at[phase],
                recv_sem=recv_sem.at[phase],
                device_id=(group, target),
                device_id_type=pl.DeviceIdType.MESH,
            ).start()

        return copy_to

    def exchange(send, recv, rows, phase, beyond=-1):
        recv[me, rows] = send[me, rows]
        farthest_first(sender(send, recv, rows, phase), beyond)

    def finish(recv, rows, phase):
        arrived = recv.at[pl.ds(0, axis_size - 1), rows]
        pltpu.make_async_copy(arrived, arrived, recv_sem.at[phase]).wait()

    def drain(send, rows, phase):
        sent = send.at[pl.ds(0, axis_size - 1), rows]
        pltpu.make_async_copy(sent, sent, send_sem.at[phase]).wait()

    def matrix(k):
        return tables[k][0], tables[k][1]

    qy, qyt, qz, qzt, qx, qxt = [lambda k=k: matrix(k) for k in range(TABLES)]

    def forward_slab(value):
        return product(qy(), split(product(split(value), qzt())))

    def backward_slab(recv, even_row, odd_row):
        spectrum = jnp.concatenate([recv[:, even_row, :], recv[:, odd_row, :]], 0)
        return product(split(product(qyt(), split(spectrum))), qz())

    def pencils(recv, rows):
        return jnp.concatenate([recv[:, row, :] for row in rows], 0)

    def forward_pencils(columns):
        return product(qx(), split(jnp.concatenate(columns, 1)))

    def potential(value):
        return value * value * value - value

    def first_row(parity, field, image, plane):
        return parity * 2 * both + (field * image_count + image) * planes + plane

    def row_of(image, parity, plane):
        return (image * 2 + parity) * planes + plane

    for load in loads:
        load.wait()
    for image in range(image_count):
        for plane in range(planes):
            value = images_ref[image, plane]
            for field, part in enumerate((value, potential(value))):
                spectrum = forward_slab(part)
                for parity in range(2):
                    first_send[:, first_row(parity, field, image, plane), :] = spectrum[parity * half : (parity + 1) * half]
    first_rows = [pl.ds(parity * 2 * both, 2 * both) for parity in range(2)]

    @pl.when(my_core == 0)
    def _():
        pl.semaphore_wait(barrier, 2 * CORES * near + 1)
        signal(told_sem.at[0], partner(0, 1))

    @pl.when(my_core == 1)
    def _():
        pl.semaphore_wait(told_sem.at[0], 1)

    copy_early = sender(first_send, first_recv, first_rows[0], 0)
    copy_early(partner(0, 1 - my_core))

    def near_step(i, carry):
        for core in (my_core, 1 - my_core):
            copy_early(partner(near - i, core))
            copy_early(partner(i - near, core))
        return carry

    lax.fori_loop(0, near, near_step, 0)

    @pl.when(my_core == 1)
    def _():
        pl.semaphore_wait(barrier, axis_size - 1)
        signal(told_sem.at[1], partner(0, 0))

    @pl.when(my_core == 0)
    def _():
        pl.semaphore_wait(told_sem.at[1], 1)

    exchange(first_send, first_recv, first_rows[0], 0, near)
    exchange(first_send, first_recv, first_rows[1], 1)

    def squares_of(index, length):
        frequency = jnp.where(index <= length // 2, index, index - length // 2).astype(jnp.float32)
        number = frequency * (2.0 * math.pi / length)
        return number * number

    square_x = squares_of(lax.broadcasted_iota(jnp.int32, (first_length, third_length), 0), first_length)
    square_z = squares_of(lax.broadcasted_iota(jnp.int32, (first_length, third_length), 1), third_length)
    my_rows = jnp.full((first_length, third_length), me, jnp.int32)
    frequencies_y = (my_rows, jnp.where(my_rows == 0, half, my_rows))
    damping, coupling = [], []
    for frequency in frequencies_y:
        number = frequency.astype(jnp.float32) * (2.0 * math.pi / second_length)
        squares = square_x + number * number + square_z
        damping.append(1.0 / (1.0 + time_step * gradient_weight * squares * squares))
        coupling.append(time_step * squares * damping[-1])

    weight = [[weights_ref[i : i + 1, j : j + 1] for j in range(image_count)] for i in range(image_count)]

    def mixed(values):
        new = []
        for i in range(image_count):
            total = weight[i][0] * values[0]
            for j in range(1, image_count):
                total = total + weight[i][j] * values[j]
            new.append(total)
        return new

    def columns_of(value, k):
        return value[:, k * third_length : (k + 1) * third_length]

    lane = lax.broadcasted_iota(jnp.int32, (1, third_length), 1)

    def spacing_parts(values, row, iteration):
        for j in range(image_count - 1):
            difference = values[j + 1] - values[j]
            row = row + jnp.where(lane == iteration * (image_count - 1) + j, jnp.sum(difference * difference), 0.0)
        return row

    parts = jnp.zeros((1, third_length), jnp.float32)
    back_chunks = [(0, pl.ds(0, planes), 2), (1, pl.ds(planes, planes), 3)] + [
        (1, pl.ds(image * 2 * planes, 2 * planes), 3 + image) for image in range(1, image_count)
    ]
    for parity in range(2):
        finish(first_recv, first_rows[parity], parity)
        spectra = forward_pencils([
            pencils(first_recv, [first_row(parity, field, image, plane) for plane in range(planes)])
            for field in range(2)
            for image in range(image_count)
        ])
        new = [
            damping[parity] * columns_of(spectra, image) - coupling[parity] * columns_of(spectra, image_count + image)
            for image in range(image_count)
        ]
        parts = spacing_parts(new, parts, 0)
        new = mixed(new)
        for image in range(image_count):
            field_spectrum[image, parity] = new[image]
        values = product(qxt(), split(jnp.concatenate(new, 1)))
        for image in range(image_count):
            for plane in range(planes):
                back_send[:, row_of(image, parity, plane), :] = columns_of(values, image)[
                    plane * axis_size : (plane + 1) * axis_size
                ]
        for chunk_parity, rows, phase in back_chunks:
            if chunk_parity == parity:
                exchange(back_send, back_recv, rows, phase)

    image_rows = [pl.ds(image * 2 * planes, 2 * planes) for image in range(image_count)]
    finish(back_recv, back_chunks[0][1], back_chunks[0][2])
    for image in range(image_count):
        finish(back_recv, back_chunks[1 + image][1], back_chunks[1 + image][2])
        for plane in range(planes):
            value = backward_slab(back_recv, row_of(image, 0, plane), row_of(image, 1, plane))
            spectrum = forward_slab(potential(value))
            for parity in range(2):
                next_send[:, row_of(image, parity, plane), :] = spectrum[parity * half : (parity + 1) * half]
        exchange(next_send, next_recv, image_rows[image], 3 + image_count + image)

    part_phase = 3 + 3 * image_count
    spectra = []
    for image in range(image_count):
        finish(next_recv, image_rows[image], 3 + image_count + image)
        changes = forward_pencils([
            pencils(next_recv, [row_of(image, parity, plane) for plane in range(planes)]) for parity in range(2)
        ])
        new = [
            damping[parity] * field_spectrum[image, parity] - coupling[parity] * columns_of(changes, parity)
            for parity in range(2)
        ]
        new = jnp.concatenate(new, 1)
        spectra.append(new)
        if image == image_count - 1:
            pair_send[...] = spacing_parts(spectra, parts, 1)
            to_other_core = pltpu.make_async_remote_copy(
                src_ref=pair_send,
                dst_ref=pair_recv,
                send_sem=send_sem.at[part_phase + 1],
                recv_sem=recv_sem.at[part_phase + 1],
                device_id=(group, partner(0, 1 - my_core)),
                device_id_type=pl.DeviceIdType.MESH,
            )
            to_other_core.start()
        values = product(qxt(), split(new))
        for parity in range(2):
            for plane in range(planes):
                last_send[:, row_of(image, parity, plane), :] = columns_of(values, parity)[
                    plane * axis_size : (plane + 1) * axis_size
                ]
        if image == image_count - 1:
            to_other_core.wait()
            part_send[...] = pair_send[...] + pair_recv[...]
            part_recv[my_chip] = part_send[...]

            def part_to(step, carry):
                pltpu.make_async_remote_copy(
                    src_ref=part_send,
                    dst_ref=part_recv.at[my_chip],
                    send_sem=send_sem.at[part_phase],
                    recv_sem=recv_sem.at[part_phase],
                    device_id=(group, partner(step, my_core)),
                    device_id_type=pl.DeviceIdType.MESH,
                ).start()
                return carry

            lax.fori_loop(1, chips, part_to, 0)
        exchange(last_send, last_recv, image_rows[image], 3 + 2 * image_count + image)

    relaxed = []
    for image in range(image_count):
        if image == image_count - 1:
            arrived = part_recv.at[pl.ds(0, chips - 1)]
            pltpu.make_async_copy(arrived, arrived, recv_sem.at[part_phase]).wait()
            cell_count = first_length * second_length * third_length
            totals = jnp.sum(part_recv[...], axis=0) / cell_count
            spacing_ref[...] = totals[:, : ITERS * (image_count - 1)]
        finish(last_recv, image_rows[image], 3 + 2 * image_count + image)
        relaxed.append([
            backward_slab(last_recv, row_of(image, 0, plane), row_of(image, 1, plane)) for plane in range(planes)
        ])
    for plane in range(planes):
        for image, value in enumerate(mixed([relaxed[j][plane] for j in range(image_count)])):
            out_ref[image, plane] = value

    for parity in range(2):
        drain(first_send, first_rows[parity], parity)
    for _, rows, phase in back_chunks:
        drain(back_send, rows, phase)
    for image in range(image_count):
        drain(next_send, image_rows[image], 3 + image_count + image)
        drain(last_send, image_rows[image], 3 + 2 * image_count + image)
    sent = part_recv.at[pl.ds(0, chips - 1)]
    pltpu.make_async_copy(sent, sent, send_sem.at[part_phase]).wait()


def two_parts(matrix):
    matrix = matrix.astype(np.float32)
    high = matrix.astype(jnp.bfloat16)
    low = (matrix - high.astype(np.float32)).astype(jnp.bfloat16)
    return np.stack([high, low])


def local(axis_size, images, weights):
    image_count, planes, second_length, third_length = images.shape
    first_length = planes * axis_size
    assert second_length == 2 * axis_size and axis_size % (2 * CORES) == 0
    assert ITERS * (image_count - 1) <= third_length
    basis_x = real_basis(first_length)
    order = np.arange(first_length).reshape(axis_size, planes).T.reshape(-1)
    basis_x = basis_x[:, order]
    basis_y, basis_z = real_basis(second_length), real_basis(third_length)
    tables = [two_parts(m) for m in (basis_y, basis_y.T, basis_z, basis_z.T, basis_x, basis_x.T)]

    rows = image_count * planes * 2
    message = lambda count: pltpu.VMEM((axis_size, count, third_length), jnp.float32)
    row = pltpu.VMEM((1, third_length), jnp.float32)
    phases = 5 + 3 * image_count
    hbm = pl.BlockSpec(memory_space=pltpu.HBM)
    vmem = pl.BlockSpec(memory_space=pltpu.VMEM)
    relaxed, spacing = pl.pallas_call(
        functools.partial(kernel, images.shape, axis_size),
        out_shape=(
            pltpu.VMEM(images.shape, jnp.float32),
            pltpu.VMEM((1, ITERS * (image_count - 1)), jnp.float32),
        ),
        in_specs=[hbm] * (2 + TABLES),
        out_specs=(vmem, vmem),
        scratch_shapes=[
            pltpu.VMEM(images.shape, jnp.float32),
            pltpu.VMEM(weights.shape, jnp.float32),
            *[pltpu.VMEM(t.shape, jnp.bfloat16) for t in tables],
            message(2 * rows), message(2 * rows),
            message(rows), message(rows), message(rows), message(rows), message(rows), message(rows),
            row, row, row, pltpu.VMEM((axis_size // CORES, 1, third_length), jnp.float32),
            pltpu.VMEM((image_count, 2, first_length, third_length), jnp.float32),
            pltpu.SemaphoreType.DMA((2 + TABLES,)),
            pltpu.SemaphoreType.DMA((phases,)),
            pltpu.SemaphoreType.DMA((phases,)),
            pltpu.SemaphoreType.REGULAR((2,)),
        ],
        compiler_params=pltpu.CompilerParams(collective_id=0, has_side_effects=True),
    )(images, weights, *[jnp.asarray(t) for t in tables])
    return relaxed, spacing.reshape(ITERS, image_count - 1)


def solution(mesh):
    return jax.shard_map(
        functools.partial(local, mesh.shape["space"]),
        mesh=mesh,
        in_specs=(P("group", "space", None, None), P("group", None)),
        out_specs=(P("group", "space", None, None), P("group", None)),
        check_vma=False,
    )
```

```python
import functools
import math

import jax
import jax.numpy as jnp
import numpy as np
from jax import lax
from jax.experimental import pallas as pl
from jax.experimental.pallas import tpu as pltpu
from jax.sharding import PartitionSpec as P

ITERS = 2
CORES = 2
TABLES = 6
NEAR = 6
time_step = 0.1
gradient_weight = 1.0


def frequencies(length):
    half = length // 2
    return np.concatenate([np.arange(half), [half], np.arange(1, half)])


def real_basis(length):
    half = length // 2
    cells = np.arange(length)
    product = np.outer(frequencies(length), cells) % length
    angles = product * (2.0 * math.pi / length)
    rows = np.where(np.arange(length)[:, None] <= half, np.cos(angles), np.sin(angles)) * math.sqrt(2.0 / length)
    rows[[0, half]] *= math.sqrt(0.5)
    return rows


def split(value):
    high = value.astype(jnp.bfloat16)
    return high, (value - high.astype(jnp.float32)).astype(jnp.bfloat16)


def product(left, right):
    dot = functools.partial(jnp.dot, preferred_element_type=jnp.float32)
    return dot(left[0], right[0]) + (dot(left[0], right[1]) + dot(left[1], right[0]))


def kernel(
    shape, axis_size,
    images_hbm, weights_hbm, *refs,
):
    tables_hbm, refs = refs[:TABLES], refs[TABLES:]
    out_ref, spacing_ref, images_ref, weights_ref = refs[:4]
    tables, refs = refs[4 : 4 + TABLES], refs[4 + TABLES :]
    (
        first_send, first_recv, back_send, back_recv, next_send, next_recv, last_send, last_recv,
        pair_send, pair_recv, total_send, total_recv, part_send, part_recv, field_spectrum, load_sem, send_sem, recv_sem, told_sem,
    ) = refs
    image_count, planes, second_length, third_length = shape
    first_length = planes * axis_size
    half = second_length // 2
    chips = axis_size // CORES
    me = lax.axis_index("space")
    group = lax.axis_index("group")
    my_chip, my_core = me // CORES, lax.rem(me, CORES)
    both = image_count * planes

    def partner(offset, core):
        return lax.rem(my_chip + offset + chips, chips) * CORES + core

    near = min(NEAR, chips // 2 - 1)

    def farthest_first(visit, beyond=-1):
        visit(partner(chips // 2, my_core))
        visit(partner(chips // 2, 1 - my_core))

        def step(i, carry):
            distance = chips // 2 - 1 - i
            visit(partner(distance, my_core))
            visit(partner(-distance, my_core))
            visit(partner(distance, 1 - my_core))
            visit(partner(-distance, 1 - my_core))
            return carry

        lax.fori_loop(0, chips // 2 - 1 - max(beyond, 0), step, 0)
        if beyond < 0:
            visit(partner(0, 1 - my_core))

    loads = [
        pltpu.make_async_copy(source, target, load_sem.at[i])
        for i, (source, target) in enumerate(
            zip((images_hbm, weights_hbm, *tables_hbm), (images_ref, weights_ref, *tables))
        )
    ]
    for load in loads:
        load.start()

    barrier = pltpu.get_barrier_semaphore()

    def signal(semaphore, target):
        pl.semaphore_signal(semaphore, inc=1, device_id=(group, target), device_id_type=pl.DeviceIdType.MESH)

    def greet(distance, core):
        signal(barrier, partner(distance, core))
        signal(barrier, partner(-distance, core))

    def greet_far(i, carry):
        greet(chips // 2 - 1 - i, 1)
        return carry

    def greet_near(i, carry):
        greet(1 + i, 0)
        greet(1 + i, 1)
        return carry

    signal(barrier, partner(chips // 2, 1))
    lax.fori_loop(0, chips // 2 - 1 - near, greet_far, 0)
    lax.fori_loop(0, near, greet_near, 0)
    signal(barrier, partner(0, 1 - my_core))
    def sender(send, recv, rows, phase):
        def copy_to(target):
            pltpu.make_async_remote_copy(
                src_ref=send.at[target, rows],
                dst_ref=recv.at[me, rows],
                send_sem=send_sem.at[phase],
                recv_sem=recv_sem.at[phase],
                device_id=(group, target),
                device_id_type=pl.DeviceIdType.MESH,
            ).start()

        return copy_to

    def exchange(send, recv, rows, phase, beyond=-1):
        recv[me, rows] = send[me, rows]
        farthest_first(sender(send, recv, rows, phase), beyond)

    def finish(recv, rows, phase):
        arrived = recv.at[pl.ds(0, axis_size - 1), rows]
        pltpu.make_async_copy(arrived, arrived, recv_sem.at[phase]).wait()

    def drain(send, rows, phase):
        sent = send.at[pl.ds(0, axis_size - 1), rows]
        pltpu.make_async_copy(sent, sent, send_sem.at[phase]).wait()

    def matrix(k):
        return tables[k][0], tables[k][1]

    qy, qyt, qz, qzt, qx, qxt = [lambda k=k: matrix(k) for k in range(TABLES)]

    def forward_slab(value):
        return product(qy(), split(product(split(value), qzt())))

    def backward_slab(recv, even_row, odd_row):
        spectrum = jnp.concatenate([recv[:, even_row, :], recv[:, odd_row, :]], 0)
        return product(split(product(qyt(), split(spectrum))), qz())

    def pencils(recv, rows):
        return jnp.concatenate([recv[:, row, :] for row in rows], 0)

    def forward_pencils(columns):
        return product(qx(), split(jnp.concatenate(columns, 1)))

    def potential(value):
        return value * value * value - value

    def first_row(parity, field, image, plane):
        return parity * 2 * both + (field * image_count + image) * planes + plane

    def row_of(image, parity, plane):
        return (image * 2 + parity) * planes + plane

    for load in loads:
        load.wait()
    for image in range(image_count):
        for plane in range(planes):
            value = images_ref[image, plane]
            for field, part in enumerate((value, potential(value))):
                spectrum = forward_slab(part)
                for parity in range(2):
                    first_send[:, first_row(parity, field, image, plane), :] = spectrum[parity * half : (parity + 1) * half]
    first_rows = [pl.ds(parity * 2 * both, 2 * both) for parity in range(2)]

    @pl.when(my_core == 0)
    def _():
        pl.semaphore_wait(barrier, 2 * CORES * near + 1)
        signal(told_sem.at[0], partner(0, 1))

    @pl.when(my_core == 1)
    def _():
        pl.semaphore_wait(told_sem.at[0], 1)

    copy_early = sender(first_send, first_recv, first_rows[0], 0)
    copy_early(partner(0, 1 - my_core))

    def near_step(i, carry):
        for core in (my_core, 1 - my_core):
            copy_early(partner(near - i, core))
            copy_early(partner(i - near, core))
        return carry

    lax.fori_loop(0, near, near_step, 0)

    @pl.when(my_core == 1)
    def _():
        pl.semaphore_wait(barrier, axis_size - 1)
        signal(told_sem.at[1], partner(0, 0))

    @pl.when(my_core == 0)
    def _():
        pl.semaphore_wait(told_sem.at[1], 1)

    exchange(first_send, first_recv, first_rows[0], 0, near)
    exchange(first_send, first_recv, first_rows[1], 1)

    def squares_of(index, length):
        frequency = jnp.where(index <= length // 2, index, index - length // 2).astype(jnp.float32)
        number = frequency * (2.0 * math.pi / length)
        return number * number

    square_x = squares_of(lax.broadcasted_iota(jnp.int32, (first_length, third_length), 0), first_length)
    square_z = squares_of(lax.broadcasted_iota(jnp.int32, (first_length, third_length), 1), third_length)
    my_rows = jnp.full((first_length, third_length), me, jnp.int32)
    frequencies_y = (my_rows, jnp.where(my_rows == 0, half, my_rows))
    damping, coupling = [], []
    for frequency in frequencies_y:
        number = frequency.astype(jnp.float32) * (2.0 * math.pi / second_length)
        squares = square_x + number * number + square_z
        damping.append(1.0 / (1.0 + time_step * gradient_weight * squares * squares))
        coupling.append(time_step * squares * damping[-1])

    weight = [[weights_ref[i : i + 1, j : j + 1] for j in range(image_count)] for i in range(image_count)]

    def mixed(values):
        new = []
        for i in range(image_count):
            total = weight[i][0] * values[0]
            for j in range(1, image_count):
                total = total + weight[i][j] * values[j]
            new.append(total)
        return new

    def columns_of(value, k):
        return value[:, k * third_length : (k + 1) * third_length]

    lane = lax.broadcasted_iota(jnp.int32, (1, third_length), 1)

    def spacing_parts(values, row, iteration):
        for j in range(image_count - 1):
            difference = values[j + 1] - values[j]
            row = row + jnp.where(lane == iteration * (image_count - 1) + j, jnp.sum(difference * difference), 0.0)
        return row

    parts = jnp.zeros((1, third_length), jnp.float32)
    back_chunks = [(0, pl.ds(0, planes), 2), (1, pl.ds(planes, planes), 3)] + [
        (1, pl.ds(image * 2 * planes, 2 * planes), 3 + image) for image in range(1, image_count)
    ]
    for parity in range(2):
        finish(first_recv, first_rows[parity], parity)
        spectra = forward_pencils([
            pencils(first_recv, [first_row(parity, field, image, plane) for plane in range(planes)])
            for field in range(2)
            for image in range(image_count)
        ])
        new = [
            damping[parity] * columns_of(spectra, image) - coupling[parity] * columns_of(spectra, image_count + image)
            for image in range(image_count)
        ]
        parts = spacing_parts(new, parts, 0)
        new = mixed(new)
        for image in range(image_count):
            field_spectrum[image, parity] = new[image]
        values = product(qxt(), split(jnp.concatenate(new, 1)))
        for image in range(image_count):
            for plane in range(planes):
                back_send[:, row_of(image, parity, plane), :] = columns_of(values, image)[
                    plane * axis_size : (plane + 1) * axis_size
                ]
        for chunk_parity, rows, phase in back_chunks:
            if chunk_parity == parity:
                exchange(back_send, back_recv, rows, phase)

    image_rows = [pl.ds(image * 2 * planes, 2 * planes) for image in range(image_count)]
    finish(back_recv, back_chunks[0][1], back_chunks[0][2])
    for image in range(image_count):
        finish(back_recv, back_chunks[1 + image][1], back_chunks[1 + image][2])
        for plane in range(planes):
            value = backward_slab(back_recv, row_of(image, 0, plane), row_of(image, 1, plane))
            spectrum = forward_slab(potential(value))
            for parity in range(2):
                next_send[:, row_of(image, parity, plane), :] = spectrum[parity * half : (parity + 1) * half]
        exchange(next_send, next_recv, image_rows[image], 3 + image_count + image)

    part_phase = 3 + 3 * image_count
    spectra = []
    for image in range(image_count):
        finish(next_recv, image_rows[image], 3 + image_count + image)
        changes = forward_pencils([
            pencils(next_recv, [row_of(image, parity, plane) for plane in range(planes)]) for parity in range(2)
        ])
        new = [
            damping[parity] * field_spectrum[image, parity] - coupling[parity] * columns_of(changes, parity)
            for parity in range(2)
        ]
        new = jnp.concatenate(new, 1)
        spectra.append(new)
        if image == image_count - 1:
            pair_send[...] = spacing_parts(spectra, parts, 1)
            to_other_core = pltpu.make_async_remote_copy(
                src_ref=pair_send,
                dst_ref=pair_recv,
                send_sem=send_sem.at[part_phase + 1],
                recv_sem=recv_sem.at[part_phase + 1],
                device_id=(group, partner(0, 1 - my_core)),
                device_id_type=pl.DeviceIdType.MESH,
            )
            to_other_core.start()
        values = product(qxt(), split(new))
        for parity in range(2):
            for plane in range(planes):
                last_send[:, row_of(image, parity, plane), :] = columns_of(values, parity)[
                    plane * axis_size : (plane + 1) * axis_size
                ]
        if image == image_count - 1:
            to_other_core.wait()
            part_send[...] = pair_send[...] + pair_recv[...]

            @pl.when(my_core == 0)
            def _():
                part_recv[0] = part_send[...]

            def part_to(step, carry):
                pltpu.make_async_remote_copy(
                    src_ref=part_send,
                    dst_ref=part_recv.at[step],
                    send_sem=send_sem.at[part_phase],
                    recv_sem=recv_sem.at[part_phase],
                    device_id=(group, partner(CORES * step + my_core, my_core)),
                    device_id_type=pl.DeviceIdType.MESH,
                ).start()
                return carry

            lax.fori_loop(1 - my_core, chips // CORES, part_to, 0)
        exchange(last_send, last_recv, image_rows[image], 3 + 2 * image_count + image)

    def wait_parts(semaphores):
        for core in range(CORES):

            @pl.when(my_core == core)
            def _():
                rows = part_recv.at[pl.ds(0, chips // CORES - 1 + core)]
                pltpu.make_async_copy(rows, rows, semaphores.at[part_phase]).wait()

    relaxed = []
    for image in range(image_count):
        if image == image_count - 1:
            wait_parts(recv_sem)
            total_send[...] = jnp.sum(part_recv[...], axis=0)
            total_to_other_core = pltpu.make_async_remote_copy(
                src_ref=total_send,
                dst_ref=total_recv,
                send_sem=send_sem.at[part_phase + 2],
                recv_sem=recv_sem.at[part_phase + 2],
                device_id=(group, partner(0, 1 - my_core)),
                device_id_type=pl.DeviceIdType.MESH,
            )
            total_to_other_core.start()
        finish(last_recv, image_rows[image], 3 + 2 * image_count + image)
        relaxed.append([
            backward_slab(last_recv, row_of(image, 0, plane), row_of(image, 1, plane)) for plane in range(planes)
        ])
    for plane in range(planes):
        for image, value in enumerate(mixed([relaxed[j][plane] for j in range(image_count)])):
            out_ref[image, plane] = value

    for parity in range(2):
        drain(first_send, first_rows[parity], parity)
    for _, rows, phase in back_chunks:
        drain(back_send, rows, phase)
    for image in range(image_count):
        drain(next_send, image_rows[image], 3 + image_count + image)
        drain(last_send, image_rows[image], 3 + 2 * image_count + image)
    wait_parts(send_sem)
    total_to_other_core.wait()
    cell_count = first_length * second_length * third_length
    totals = (total_send[...] + total_recv[...]) / cell_count
    spacing_ref[...] = totals[:, : ITERS * (image_count - 1)]


def two_parts(matrix):
    matrix = matrix.astype(np.float32)
    high = matrix.astype(jnp.bfloat16)
    low = (matrix - high.astype(np.float32)).astype(jnp.bfloat16)
    return np.stack([high, low])


def local(axis_size, images, weights):
    image_count, planes, second_length, third_length = images.shape
    first_length = planes * axis_size
    assert second_length == 2 * axis_size and axis_size % (2 * CORES) == 0
    assert ITERS * (image_count - 1) <= third_length
    basis_x = real_basis(first_length)
    order = np.arange(first_length).reshape(axis_size, planes).T.reshape(-1)
    basis_x = basis_x[:, order]
    basis_y, basis_z = real_basis(second_length), real_basis(third_length)
    tables = [two_parts(m) for m in (basis_y, basis_y.T, basis_z, basis_z.T, basis_x, basis_x.T)]

    rows = image_count * planes * 2
    message = lambda count: pltpu.VMEM((axis_size, count, third_length), jnp.float32)
    row = pltpu.VMEM((1, third_length), jnp.float32)
    phases = 6 + 3 * image_count
    hbm = pl.BlockSpec(memory_space=pltpu.HBM)
    vmem = pl.BlockSpec(memory_space=pltpu.VMEM)
    relaxed, spacing = pl.pallas_call(
        functools.partial(kernel, images.shape, axis_size),
        out_shape=(
            pltpu.VMEM(images.shape, jnp.float32),
            pltpu.VMEM((1, ITERS * (image_count - 1)), jnp.float32),
        ),
        in_specs=[hbm] * (2 + TABLES),
        out_specs=(vmem, vmem),
        scratch_shapes=[
            pltpu.VMEM(images.shape, jnp.float32),
            pltpu.VMEM(weights.shape, jnp.float32),
            *[pltpu.VMEM(t.shape, jnp.bfloat16) for t in tables],
            message(2 * rows), message(2 * rows),
            message(rows), message(rows), message(rows), message(rows), message(rows), message(rows),
            row, row, row, row, row, pltpu.VMEM((axis_size // CORES // CORES, 1, third_length), jnp.float32),
            pltpu.VMEM((image_count, 2, first_length, third_length), jnp.float32),
            pltpu.SemaphoreType.DMA((2 + TABLES,)),
            pltpu.SemaphoreType.DMA((phases,)),
            pltpu.SemaphoreType.DMA((phases,)),
            pltpu.SemaphoreType.REGULAR((2,)),
        ],
        compiler_params=pltpu.CompilerParams(collective_id=0, has_side_effects=True),
    )(images, weights, *[jnp.asarray(t) for t in tables])
    return relaxed, spacing.reshape(ITERS, image_count - 1)


def solution(mesh):
    return jax.shard_map(
        functools.partial(local, mesh.shape["space"]),
        mesh=mesh,
        in_specs=(P("group", "space", None, None), P("group", None)),
        out_specs=(P("group", "space", None, None), P("group", None)),
        check_vma=False,
    )
```
